8 devices in a mesh: rep: 1 (over z), tp: 2 (over y), sp: 4 (over x, core).
Axes of the slice: x: 2, y: 2, z: 1, core: 2. Of those that a mesh axis runs over, the one named last changes fastest.
Arguments:
- x_tokens: bfloat16 [8192, 3840], P(('rep', 'sp'))
- positions: int32 [8192], P(('rep', 'sp'))
- gains: float32 [2, 4, 3840], replicated
- w_q: bfloat16 [2, 3840, 16, 256], P(None, None, 'tp')
- w_k: bfloat16 [2, 3840, 8, 256], P(None, None, 'tp')
- w_v: bfloat16 [2, 3840, 8, 256], P(None, None, 'tp')
- w_o: bfloat16 [2, 16, 256, 3840], P(None, 'tp')
- w_gate: bfloat16 [2, 3840, 15360], P(None, None, 'tp')
- w_up: bfloat16 [2, 3840, 15360], P(None, None, 'tp')
- w_down: bfloat16 [2, 15360, 3840], P(None, 'tp')
Outputs:
- output 1: bfloat16 [8192, 3840], P(('rep', 'sp'))
- output 2: bfloat16 [512, 8, 256], P('rep', ('tp', 'sp'))
- output 3: bfloat16 [512, 8, 256], P('rep', ('tp', 'sp'))
- output 4: bfloat16 [8192, 8, 256], P('rep', ('tp', 'sp'))
- output 5: bfloat16 [8192, 8, 256], P('rep', ('tp', 'sp'))
All inputs are finite; a program needn't handle non-finite values.
Results may differ from the reference program's by a relative error of at most 0.0163675.
Values are sent between devices in bfloat16 or wider.
A program may use at most 2 GiB of HBM per device.

```python
import jax
import jax.numpy as jnp
from jax import lax

D = 3840
HEADS = 16
KV_HEADS = 8
HEAD = 256
FF = 15360
TOKENS = 8192
WINDOW = 512
CACHE_HEADS = 8
REF_BLOCK = 64

GROUP_SIZE = HEADS // KV_HEADS
REPEAT = CACHE_HEADS // KV_HEADS
NORM_EPS = 1e-6
LOCAL_BASE = 10000.0
GLOBAL_BASE = 1000000.0


def setup_inputs(seed: int = 0, part: int = 0) -> dict:
    part_key = jax.random.fold_in(jax.random.key(seed), part)
    key_x, key_pos = jax.random.split(part_key, 2)
    weight_keys = jax.random.split(jax.random.key(seed + 1), 8)
    x_tokens = jax.random.normal(key_x, (TOKENS, D), jnp.float32).astype(jnp.bfloat16)
    start = jax.random.randint(key_pos, (), 0, 4096)
    positions = (start + jnp.arange(TOKENS)).astype(jnp.int32)
    gains = 1.0 + 0.25 * jax.random.normal(weight_keys[0], (2, 4, D), jnp.float32)

    def weight(key, shape, fan_in):
        return (jax.random.normal(key, shape, jnp.float32) * fan_in ** -0.5).astype(jnp.bfloat16)

    return {
        'x_tokens': x_tokens,
        'positions': positions,
        'gains': gains,
        'w_q': weight(weight_keys[1], (2, D, HEADS, HEAD), D),
        'w_k': weight(weight_keys[2], (2, D, KV_HEADS, HEAD), D),
        'w_v': weight(weight_keys[3], (2, D, KV_HEADS, HEAD), D),
        'w_o': weight(weight_keys[4], (2, HEADS, HEAD, D), HEADS * HEAD),
        'w_gate': weight(weight_keys[5], (2, D, FF), D),
        'w_up': weight(weight_keys[6], (2, D, FF), D),
        'w_down': weight(weight_keys[7], (2, FF, D), FF),
    }


def rms_norm(values, gain):
    wide = values.astype(jnp.float32)
    inv_rms = lax.rsqrt(jnp.mean(wide * wide, axis=-1, keepdims=True) + NORM_EPS)
    return wide * inv_rms * gain


def rotary(projected, positions, base):
    half = projected.shape[-1] // 2
    inv_freq = base ** (-jnp.arange(half, dtype=jnp.float32) / half)
    angles = positions.astype(jnp.float32)[..., None] * inv_freq
    cos_part = jnp.cos(angles)[..., None, :]
    sin_part = jnp.sin(angles)[..., None, :]
    first = projected[..., :half]
    second = projected[..., half:]
    return jnp.concatenate([first * cos_part - second * sin_part, second * cos_part + first * sin_part], axis=-1)


def attention(q_rot, k_rot, v_new, local):
    q_wide = q_rot.reshape(TOKENS, KV_HEADS, GROUP_SIZE, HEAD).astype(jnp.float32)
    k_wide = k_rot.astype(jnp.float32)
    v_wide = v_new.astype(jnp.float32)
    span = WINDOW + REF_BLOCK if local else TOKENS

    def one_block(block_id):
        q_start = block_id * REF_BLOCK
        q_tile = lax.dynamic_slice_in_dim(q_wide, q_start, REF_BLOCK, 0)
        q_idx = q_start + jnp.arange(REF_BLOCK)
        k_start = jnp.clip(q_start - WINDOW, 0, TOKENS - span) if local else 0
        k_tile = lax.dynamic_slice_in_dim(k_wide, k_start, span, 0)
        v_tile = lax.dynamic_slice_in_dim(v_wide, k_start, span, 0)
        k_idx = k_start + jnp.arange(span)
        allowed = k_idx[None, :] <= q_idx[:, None]
        if local:
            allowed = allowed & (q_idx[:, None] - k_idx[None, :] < WINDOW)
        scores = jnp.einsum('qhgd,khd->hgqk', q_tile, k_tile) * (HEAD ** -0.5)
        weights = jax.nn.softmax(jnp.where(allowed, scores, -1e30), axis=-1)
        weights = weights.astype(jnp.bfloat16).astype(jnp.float32)
        return jnp.einsum('hgqk,khd->qhgd', weights, v_tile).astype(jnp.bfloat16)

    blocks = lax.map(one_block, jnp.arange(TOKENS // REF_BLOCK))
    return blocks.reshape(TOKENS, HEADS * HEAD)


def layer(hidden, positions, gain, w_q, w_k, w_v, w_o, w_gate, w_up, w_down, local):
    base = LOCAL_BASE if local else GLOBAL_BASE
    u_norm = rms_norm(hidden, gain[0]).astype(jnp.bfloat16)
    q_proj = jnp.dot(u_norm, w_q.reshape(D, HEADS * HEAD), preferred_element_type=jnp.float32)
    k_proj = jnp.dot(u_norm, w_k.reshape(D, KV_HEADS * HEAD), preferred_element_type=jnp.float32)
    v_proj = jnp.dot(u_norm, w_v.reshape(D, KV_HEADS * HEAD), preferred_element_type=jnp.float32)
    q_rot = rotary(q_proj.reshape(TOKENS, HEADS, HEAD), positions, base).astype(jnp.bfloat16)
    k_rot = rotary(k_proj.reshape(TOKENS, KV_HEADS, HEAD), positions, base).astype(jnp.bfloat16)
    v_new = v_proj.reshape(TOKENS, KV_HEADS, HEAD).astype(jnp.bfloat16)
    attn_out = attention(q_rot, k_rot, v_new, local)
    o_sum = jnp.dot(attn_out, w_o.reshape(HEADS * HEAD, D), preferred_element_type=jnp.float32)
    x_mid = (hidden.astype(jnp.float32) + rms_norm(o_sum, gain[1])).astype(jnp.bfloat16)
    u_mlp = rms_norm(x_mid, gain[2]).astype(jnp.bfloat16)
    gate_pre = jnp.dot(u_mlp, w_gate, preferred_element_type=jnp.float32)
    up_pre = jnp.dot(u_mlp, w_up, preferred_element_type=jnp.float32)
    hidden_act = (jax.nn.silu(gate_pre) * up_pre).astype(jnp.bfloat16)
    m_sum = jnp.dot(hidden_act, w_down, preferred_element_type=jnp.float32)
    x_out = (x_mid.astype(jnp.float32) + rms_norm(m_sum, gain[3])).astype(jnp.bfloat16)
    k_cache = jnp.repeat(k_rot, REPEAT, axis=1)
    v_cache = jnp.repeat(v_new, REPEAT, axis=1)
    if local:
        return x_out, k_cache[TOKENS - WINDOW:], v_cache[TOKENS - WINDOW:]
    return x_out, k_cache, v_cache


def reference(x_tokens, positions, gains, w_q, w_k, w_v, w_o, w_gate, w_up, w_down):
    hidden, k_local, v_local = layer(x_tokens, positions, gains[0], w_q[0], w_k[0], w_v[0], w_o[0], w_gate[0], w_up[0], w_down[0], True)
    out_hidden, k_global, v_global = layer(hidden, positions, gains[1], w_q[1], w_k[1], w_v[1], w_o[1], w_gate[1], w_up[1], w_down[1], False)
    return out_hidden, k_local, v_local, k_global, v_global
```

```python
import functools
import math

import jax
import jax.numpy as jnp
from jax import lax
from jax.experimental import pallas as pl
from jax.experimental.pallas import tpu as pltpu
from jax.sharding import PartitionSpec as P


NORM_EPS = 1e-6
WINDOW = 512
LOCAL_BASE = 10000.0
GLOBAL_BASE = 1000000.0
CHUNK = 512
HALF = CHUNK // 2
HEAD = 256
NEG = -1e30
VMEM = 62 * 1024 * 1024
BF16 = jnp.bfloat16
F32 = jnp.float32


def cost(flops, nbytes):
    return pl.CostEstimate(flops=int(flops), bytes_accessed=int(nbytes), transcendentals=0)


def call(kernel, grid, in_specs, out_specs, out_shape, args, scalars=(), scratch=(), after=(), aliases=None, cost_estimate=None):
    first = len(scalars) + len(in_specs)
    extra = len(after)
    wrapped = lambda *refs: kernel(*refs[:first], *refs[first + extra:])
    return pl.pallas_call(
        wrapped,
        grid_spec=pltpu.PrefetchScalarGridSpec(
            num_scalar_prefetch=len(scalars), grid=grid, in_specs=list(in_specs) + [pl.BlockSpec(memory_space=pl.ANY)] * extra,
            out_specs=out_specs, scratch_shapes=scratch),
        out_shape=out_shape, cost_estimate=cost_estimate, input_output_aliases=aliases or {},
        compiler_params=pltpu.CompilerParams(dimension_semantics=('arbitrary',) * len(grid), vmem_limit_bytes=VMEM))(
            *scalars, *args, *after)


LANES = 128


def tiles(width):
    return [slice(i * LANES, (i + 1) * LANES) for i in range(width // LANES)]


def row_blocks(rows, size, fn):
    def body(i, carry):
        fn(pl.multiple_of(i * size, size))
        return carry

    lax.fori_loop(0, rows // size, body, 0)


def to_inv_rms(sums_ref, rows, width):
    mean = jnp.sum(sums_ref[:rows], axis=1, keepdims=True) * (1.0 / width)
    sums_ref[:rows] = jnp.broadcast_to(lax.rsqrt(mean + NORM_EPS), (rows, LANES))


REGROUP_ROWS = 128


def regroup_kernel(q_ref, k_ref, v_ref, o_ref):
    def pick(heads):
        depth = HEAD // heads
        row = lax.broadcasted_iota(jnp.int32, (HEAD, HEAD), 0)
        col = lax.broadcasted_iota(jnp.int32, (HEAD, HEAD), 1)
        return (lax.rem(row, depth) * heads + row // depth == col).astype(BF16)

    rows = o_ref.shape[0]
    groups = k_ref.shape[2]
    per = q_ref.shape[2] // groups
    width = (per + 2) * HEAD
    for ref, first, count in ((q_ref, 0, per), (k_ref, per, 1), (v_ref, per + 1, 1)):
        heads = groups * count
        depth = HEAD // heads
        order = pick(heads)
        for b in range(rows // depth):
            block = ref[0, b * depth:(b + 1) * depth].reshape(HEAD, HEAD)
            out = jnp.dot(order, block, preferred_element_type=F32).astype(BF16)
            for h in range(heads):
                base = h // count * width + (first + h % count) * HEAD
                o_ref[b * depth:(b + 1) * depth, base:base + HEAD] = out[h * depth:(h + 1) * depth]


def regroup(w_q, w_k, w_v, layer, after):
    depth = w_q.shape[1]
    cols = (w_q.shape[2] + 2 * w_k.shape[2]) * HEAD
    rows = REGROUP_ROWS
    spec = lambda w: pl.BlockSpec((1, rows, w.shape[2], HEAD), lambda i: (layer, i, 0, 0))
    return call(regroup_kernel, (depth // rows,), [spec(w_q), spec(w_k), spec(w_v)],
                pl.BlockSpec((rows, cols), lambda i: (i, 0)), jax.ShapeDtypeStruct((depth, cols), BF16),
                (w_q, w_k, w_v), after=after, cost_estimate=cost(depth * cols * 512, depth * cols * 4))


def norm_rows(x_ref, gain_ref, u_ref, sums_ref, start, rows):
    width = x_ref.shape[1]

    def squares(r):
        at = pl.ds(r, 16)
        total = None
        for cols in tiles(width):
            wide = x_ref[at, cols].astype(F32)
            total = wide * wide if total is None else total + wide * wide
        sums_ref[at, :] = total

    def apply(r):
        at = pl.ds(r, 16)
        inv = sums_ref[at, :]
        for cols in tiles(width):
            u_ref[pl.ds(start + r, 16), cols] = (x_ref[at, cols].astype(F32) * inv * gain_ref[:, cols]).astype(BF16)

    row_blocks(rows, 16, squares)
    to_inv_rms(sums_ref, rows, width)
    row_blocks(rows, 16, apply)


def rope_cols(acc, cos, sin):
    half = HEAD // 2
    a, b = acc[:, :half], acc[:, half:]
    return jnp.concatenate([a * cos - b * sin, b * cos + a * sin], axis=1).astype(BF16)


def qkv0_kernel(x_ref, gain_ref, cos_ref, sin_ref, w_ref, q_ref, kv_ref, u_ref, sums_ref):
    n, m = pl.program_id(0), pl.program_id(1)
    start = pl.multiple_of(m * CHUNK, CHUNK)

    @pl.when(n == 0)
    def _():
        norm_rows(x_ref, gain_ref, u_ref, sums_ref, start, CHUNK)

    acc = jnp.dot(u_ref[pl.ds(start, CHUNK), :], w_ref[...], preferred_element_type=F32)
    cos, sin = cos_ref[...], sin_ref[...]
    per = q_ref.shape[1] // HEAD
    for i in range(per):
        q_ref[:, i * HEAD:(i + 1) * HEAD] = rope_cols(acc[:, i * HEAD:(i + 1) * HEAD], cos, sin)
    kv_ref[:, :HEAD] = rope_cols(acc[:, per * HEAD:(per + 1) * HEAD], cos, sin)
    kv_ref[:, HEAD:] = acc[:, (per + 1) * HEAD:].astype(BF16)


def qkv0(x, gain, cos, sin, w, groups, first, count, after):
    depth, cols = w.shape
    width = cols // groups
    per = width // HEAD - 2
    last = first + count - 1
    hold = lambda n, m: (jnp.where(n == 0, first + m, last), 0)
    rows = lambda n, m: (first + m, 0)
    return call(
        qkv0_kernel, (groups, count),
        [pl.BlockSpec((CHUNK, depth), hold), pl.BlockSpec((1, depth), lambda n, m: (0, 0)),
         pl.BlockSpec((CHUNK, HEAD // 2), rows), pl.BlockSpec((CHUNK, HEAD // 2), rows),
         pl.BlockSpec((depth, width), lambda n, m: (0, n))],
        [pl.BlockSpec((CHUNK, per * HEAD), lambda n, m: (m, n)), pl.BlockSpec((CHUNK, 2 * HEAD), lambda n, m: (m, n))],
        [jax.ShapeDtypeStruct((count * CHUNK, groups * per * HEAD), BF16),
         jax.ShapeDtypeStruct((count * CHUNK, groups * 2 * HEAD), BF16)],
        (x, gain, cos, sin, w), scratch=[pltpu.VMEM((count * CHUNK, depth), BF16), pltpu.VMEM((CHUNK, LANES), F32)], after=after,
        cost_estimate=cost(2 * count * CHUNK * depth * cols, 2 * depth * cols + 4 * count * CHUNK * depth))


def qkv1_kernel(idx_ref, own_ref, peer_ref, gain_ref, cos_ref, sin_ref, w_ref, *rest):
    *out_refs, u_ref, sums_ref = rest
    n = pl.program_id(0)

    @pl.when(n == 0)
    def _():
        t = idx_ref[1]
        norm_rows(own_ref, gain_ref, u_ref, sums_ref, pl.multiple_of(t * HALF, HALF), HALF)
        norm_rows(peer_ref, gain_ref, u_ref, sums_ref, pl.multiple_of((1 - t) * HALF, HALF), HALF)

    acc = jnp.dot(u_ref[...], w_ref[...], preferred_element_type=F32)
    cos, sin = cos_ref[...], sin_ref[...]
    heads = acc.shape[1] // HEAD
    parts = [rope_cols(acc[:, i * HEAD:(i + 1) * HEAD], cos, sin) for i in range(heads - 1)]
    parts.append(acc[:, (heads - 1) * HEAD:].astype(BF16))
    for k, out_ref in enumerate(out_refs):
        @pl.when(n == k)
        def _():
            for i, part in enumerate(parts):
                out_ref[:, i * HEAD:(i + 1) * HEAD] = part


def qkv1(idx, own, peer, gain, cos, sin, w, groups, chunk, after):
    depth, cols = w.shape
    width = cols // groups
    whole = lambda n, idx: (0, 0)
    angle_spec = pl.BlockSpec((CHUNK, HEAD // 2), lambda n, idx: (chunk, 0))
    return call(
        qkv1_kernel, (groups,),
        [pl.BlockSpec((HALF, depth), whole), pl.BlockSpec((HALF, depth), whole), pl.BlockSpec((1, depth), whole),
         angle_spec, angle_spec, pl.BlockSpec((depth, width), lambda n, idx: (0, lax.rem(idx[0] + n, groups)))],
        [pl.BlockSpec((CHUNK, width), whole)] * groups, [jax.ShapeDtypeStruct((CHUNK, width), BF16)] * groups,
        (own, peer, gain, cos, sin, w), scalars=(idx,),
        scratch=[pltpu.VMEM((CHUNK, depth), BF16), pltpu.VMEM((HALF, LANES), F32)], after=after,
        cost_estimate=cost(2 * CHUNK * depth * cols, 2 * depth * cols))


def local_kernel(chunk, idx_ref, q_ref, prev_ref, kv_ref, o_ref):
    lead = jnp.where((idx_ref[0] == 0) & (chunk == 0), CHUNK, 0)
    per = q_ref.shape[1] // HEAD
    scale2 = HEAD ** -0.5 * math.log2(math.e)
    size = CHUNK // 2
    span = WINDOW + size
    for tile in range(CHUNK // size):
        low = tile * size
        q = jnp.concatenate([q_ref[low:low + size, i * HEAD:(i + 1) * HEAD] for i in range(per)], axis=0)
        k = jnp.concatenate([prev_ref[low:, :HEAD], kv_ref[:low + size, :HEAD]], axis=0)
        v = jnp.concatenate([prev_ref[low:, HEAD:], kv_ref[:low + size, HEAD:]], axis=0)
        s = lax.dot_general(q, k, (((1,), (1,)), ((), ())), preferred_element_type=F32)
        row = lax.rem(lax.broadcasted_iota(jnp.int32, (per * size, span), 0), size)
        key = lax.broadcasted_iota(jnp.int32, (per * size, span), 1)
        allowed = (key > row) & (key <= row + WINDOW) & (key >= lead - low)
        s = jnp.where(allowed, s, NEG)
        p = jnp.exp2((s - jnp.max(s, axis=1, keepdims=True)) * scale2)
        weights = (p * (1.0 / jnp.sum(p, axis=1, keepdims=True))).astype(BF16)
        out = jnp.dot(weights, v, preferred_element_type=F32).astype(BF16)
        for i in range(per):
            o_ref[low:low + size, i * HEAD:(i + 1) * HEAD] = out[i * size:(i + 1) * size]


def local_attention(idx, q, prev, kv, groups, chunk, after):
    per = q.shape[1] // groups // HEAD
    block = lambda width: pl.BlockSpec((CHUNK, width * HEAD), lambda g, idx: (0, g))
    return call(
        functools.partial(local_kernel, chunk), (groups,), [block(per), block(2), block(2)],
        block(per), jax.ShapeDtypeStruct((CHUNK, q.shape[1]), BF16), (q, prev, kv), scalars=(idx,), after=after,
        cost_estimate=cost(12 * CHUNK * q.shape[1] * WINDOW, 10 * CHUNK * q.shape[1]))


def global_kernel(chunk, chunks, groups, emit, idx_ref, *refs):
    q_refs, refs = refs[:groups], refs[groups:]
    src_refs, refs = refs[:chunks * groups], refs[chunks * groups:]
    out_refs, refs = refs[:groups], refs[groups:]
    if emit:
        k_out, v_out, *refs = refs
    k_all, v_all, q_all, s_ref, m_ref, l_ref, acc_ref, sems, out_sem = refs
    s = idx_ref[0]
    per = out_refs[0].shape[1] // HEAD
    rows = per * CHUNK
    scale2 = HEAD ** -0.5 * math.log2(math.e)
    lanes = 128
    held = chunks * CHUNK
    source = [lax.rem(s - k + groups, groups) for k in range(groups)]

    copies = []
    for c in range(chunks):
        for k in range(groups):
            at = pl.ds(pl.multiple_of(source[k] * held + c * CHUNK, CHUNK), CHUNK)
            ref = src_refs[c * groups + k]
            for j, dst in ((per, k_all), (per + 1, v_all)):
                copy = pltpu.make_async_copy(ref.at[:, pl.ds(j * HEAD, HEAD)], dst.at[at, :], sems)
                copy.start()
                copies.append(copy)
    for copy in copies:
        copy.wait()
    if emit:
        outs = [pltpu.make_async_copy(k_all, k_out, out_sem.at[0]), pltpu.make_async_copy(v_all, v_out, out_sem.at[1])]
        for copy in outs:
            copy.start()

    def scores(block):
        at = pl.ds(pl.multiple_of(block * CHUNK, CHUNK), CHUNK)
        return lax.dot_general(q_all[...], k_all[at, :], (((1,), (1,)), ((), ())), preferred_element_type=F32)

    def soften(sc, block):
        top = jnp.max(sc, axis=1, keepdims=True)
        before = m_ref[...]
        now = jnp.maximum(before, top)
        m_ref[...] = now
        alpha = jnp.exp2((before - now) * scale2)
        parts = [jnp.exp2((sc[:, i * lanes:(i + 1) * lanes] - now) * scale2) for i in range(CHUNK // lanes)]
        total = parts[0]
        for part in parts[1:]:
            total = total + part
        l_ref[...] = l_ref[...] * alpha + total
        p = jnp.concatenate([part.astype(BF16) for part in parts], axis=1)
        at = pl.ds(pl.multiple_of(block * CHUNK, CHUNK), CHUNK)
        pv = jnp.dot(p, v_all[at, :], preferred_element_type=F32)
        for i in range(HEAD // lanes):
            cols = slice(i * lanes, (i + 1) * lanes)
            acc_ref[:, cols] = acc_ref[:, cols] * alpha + pv[:, cols]

    for k in range(groups):
        for i in range(per):
            q_all[i * CHUNK:(i + 1) * CHUNK, :] = q_refs[k][:, i * HEAD:(i + 1) * HEAD]
        m_ref[...] = jnp.full((rows, lanes), NEG, F32)
        l_ref[...] = jnp.zeros((rows, lanes), F32)
        acc_ref[...] = jnp.zeros((rows, HEAD), F32)
        full = source[k] * chunks + chunk
        s_ref[...] = scores(0)

        def body(block, carry):
            current = s_ref[...]
            following = scores(block + 1)
            soften(current, block)
            s_ref[...] = following
            return carry

        lax.fori_loop(0, full, body, 0)
        row = lax.rem(lax.broadcasted_iota(jnp.int32, (rows, CHUNK), 0), CHUNK)
        key = lax.broadcasted_iota(jnp.int32, (rows, CHUNK), 1)
        soften(jnp.where(key <= row, s_ref[...], NEG), full)
        scale = 1.0 / jnp.sum(l_ref[...], axis=1, keepdims=True)
        out = (acc_ref[...] * scale).astype(BF16)
        for i in range(per):
            out_refs[k][:, i * HEAD:(i + 1) * HEAD] = out[i * CHUNK:(i + 1) * CHUNK]
    if emit:
        for copy in outs:
            copy.wait()


def global_attention(idx, received, chunk, emit, after):
    chunks, groups = len(received), len(received[0])
    per = received[0][0].shape[1] // HEAD - 2
    total = groups * chunks * CHUNK
    rows = per * CHUNK
    any_spec = pl.BlockSpec(memory_space=pl.ANY)
    whole = lambda i, idx: (0, 0)
    out_specs = [pl.BlockSpec((CHUNK, per * HEAD), whole)] * groups
    out_shape = [jax.ShapeDtypeStruct((CHUNK, per * HEAD), BF16)] * groups
    if emit:
        out_specs += [any_spec] * 2
        out_shape += [jax.ShapeDtypeStruct((total, HEAD), BF16)] * 2
    return call(
        functools.partial(global_kernel, chunk, chunks, groups, emit), (1,),
        [pl.BlockSpec((CHUNK, per * HEAD), whole)] * groups + [any_spec] * (chunks * groups), out_specs, out_shape,
        (*received[chunk], *[r for row in received for r in row]), scalars=(idx,),
        scratch=[pltpu.VMEM((total, HEAD), BF16), pltpu.VMEM((total, HEAD), BF16), pltpu.VMEM((rows, HEAD), BF16),
                 pltpu.VMEM((rows, CHUNK), F32), pltpu.VMEM((rows, LANES), F32), pltpu.VMEM((rows, LANES), F32),
                 pltpu.VMEM((rows, HEAD), F32), pltpu.SemaphoreType.DMA(()), pltpu.SemaphoreType.DMA((2,))],
        after=after, cost_estimate=cost(4 * rows * total * HEAD * groups // 2, 4 * total * HEAD))


def o_kernel(groups, split, idx_ref, *refs):
    a_refs, refs = refs[:2 * groups], refs[2 * groups:]
    w_refs, refs = refs[:2 * groups], refs[2 * groups:]
    res_refs, refs = refs[:1 + split], refs[1 + split:]
    gain1_ref, gain2_ref, h_ref, u_ref, acc_ref, sums_ref = refs
    n = pl.program_id(0)

    @pl.when(n == 0)
    def _():
        sums_ref[...] = jnp.zeros(sums_ref.shape, F32)

    total = None
    for a_ref, w_ref in zip(a_refs, w_refs):
        part = jnp.dot(a_ref[...], w_ref[...].reshape(w_ref.shape[-2:]), preferred_element_type=F32)
        total = part if total is None else total + part
    width = total.shape[1]
    acc_ref[:, pl.ds(pl.multiple_of(n * width, LANES), width)] = total
    square = total * total
    sums = sums_ref[...]
    for cols in tiles(width):
        sums = sums + square[:, cols]
    sums_ref[...] = sums

    @pl.when(n == pl.num_programs(0) - 1)
    def _():
        depth = acc_ref.shape[1]
        to_inv_rms(sums_ref, CHUNK, depth)

        def residual(res_ref, start, rows):
            def block(r):
                at = pl.ds(start + r, 16)
                inv = sums_ref[at, :]
                squares = None
                for cols in tiles(depth):
                    mid = (res_ref[pl.ds(r, 16), cols].astype(F32) + acc_ref[at, cols] * inv * gain1_ref[:, cols]).astype(BF16)
                    h_ref[at, cols] = mid
                    wide = mid.astype(F32)
                    squares = wide * wide if squares is None else squares + wide * wide
                sums_ref[at, :] = squares

            row_blocks(rows, 16, block)

        if split:
            t = idx_ref[1]
            residual(res_refs[0], pl.multiple_of(t * HALF, HALF), HALF)
            residual(res_refs[1], pl.multiple_of((1 - t) * HALF, HALF), HALF)
        else:
            residual(res_refs[0], 0, CHUNK)
        to_inv_rms(sums_ref, CHUNK, depth)

        def scale(r):
            at = pl.ds(r, 16)
            inv = sums_ref[at, :]
            for cols in tiles(depth):
                u_ref[at, cols] = (h_ref[at, cols].astype(F32) * inv * gain2_ref[:, cols]).astype(BF16)

        row_blocks(CHUNK, 16, scale)


def o_project(idx, own, peer, w_o, layer, w_peer, residual, chunk, gain1, gain2, after):
    groups = len(w_peer)
    rows, width = w_peer[0].shape
    cols = 768 if width % 768 == 0 else width
    group = lambda k: lambda idx: lax.rem(idx[0] + k, groups)
    a_specs, arrays = [], []
    for a in (own, peer):
        for k in range(groups):
            if isinstance(a, (list, tuple)):
                a_specs.append(pl.BlockSpec((CHUNK, rows), lambda n, idx: (0, 0)))
                arrays.append(a[k])
            else:
                a_specs.append(pl.BlockSpec((CHUNK, rows), lambda n, idx, g=group(k): (0, g(idx))))
                arrays.append(a)
    w_specs = [pl.BlockSpec((1, 1, rows, cols), lambda n, idx, g=group(k): (layer, g(idx), 0, n)) for k in range(groups)]
    w_specs += [pl.BlockSpec((rows, cols), lambda n, idx: (0, n))] * groups
    split = isinstance(residual, (list, tuple))
    if split:
        res_specs, res = [pl.BlockSpec((HALF, width), lambda n, idx: (0, 0))] * 2, list(residual)
    else:
        res_specs, res = [pl.BlockSpec((CHUNK, width), lambda n, idx: (chunk, 0))], [residual]
    gain_spec = pl.BlockSpec((1, width), lambda n, idx: (0, 0))
    out_spec = pl.BlockSpec((CHUNK, width), lambda n, idx: (0, 0))
    return call(
        functools.partial(o_kernel, groups, split), (width // cols,),
        a_specs + w_specs + res_specs + [gain_spec, gain_spec], [out_spec, out_spec],
        [jax.ShapeDtypeStruct((CHUNK, width), BF16)] * 2, (*arrays, *([w_o] * groups), *w_peer, *res, gain1, gain2), scalars=(idx,),
        scratch=[pltpu.VMEM((CHUNK, width), F32), pltpu.VMEM((CHUNK, LANES), F32)], after=after,
        cost_estimate=cost(4 * CHUNK * groups * rows * width, 4 * groups * rows * width))


def mlp_step(u_ref, gate_ref, up_ref, down_ref, acc_ref):
    @pl.when(pl.program_id(0) == 0)
    def _():
        acc_ref[...] = jnp.zeros(acc_ref.shape, F32)

    u = u_ref[...]
    gate = jnp.dot(u, gate_ref[0], preferred_element_type=F32)
    up = jnp.dot(u, up_ref[0], preferred_element_type=F32)
    act = (jax.nn.silu(gate) * up).astype(BF16)
    acc_ref[...] += jnp.dot(act, down_ref[0], preferred_element_type=F32)


def mlp_kernel(idx_ref, u_ref, gate_ref, up_ref, down_ref, own_ref, peer_ref, acc_ref):
    mlp_step(u_ref, gate_ref, up_ref, down_ref, acc_ref)

    @pl.when(pl.program_id(0) == pl.num_programs(0) - 1)
    def _():
        t = idx_ref[1]
        own_ref[...] = acc_ref[pl.ds(pl.multiple_of(t * HALF, HALF), HALF), :]
        peer_ref[...] = acc_ref[pl.ds(pl.multiple_of((1 - t) * HALF, HALF), HALF), :]


def mlp_half_kernel(idx_ref, u_ref, gate_ref, up_ref, down_ref, out_ref):
    mlp_step(u_ref, gate_ref, up_ref, down_ref, out_ref)


def mlp(idx, u, w_gate, w_up, w_down, layer, after, half=None):
    depth, hidden = w_gate.shape[1:]
    block = 512
    whole = lambda n, idx: (0, 0)
    in_spec = pl.BlockSpec((1, depth, block), lambda n, idx: (layer, 0, n))
    w_specs = [in_spec, in_spec, pl.BlockSpec((1, block, depth), lambda n, idx: (layer, n, 0))]
    shape = jax.ShapeDtypeStruct((HALF, depth), F32)
    if half is None:
        return call(mlp_kernel, (hidden // block,), [pl.BlockSpec((CHUNK, depth), whole)] + w_specs,
                    [pl.BlockSpec((HALF, depth), whole)] * 2, [shape] * 2, (u, w_gate, w_up, w_down), scalars=(idx,),
                    scratch=[pltpu.VMEM((CHUNK, depth), F32)], after=after,
                    cost_estimate=cost(6 * CHUNK * depth * hidden, 6 * depth * hidden))
    place = (lambda n, idx: (idx[1], 0)) if half == 'own' else (lambda n, idx: (1 - idx[1], 0))
    return call(mlp_half_kernel, (hidden // block,), [pl.BlockSpec((HALF, depth), place)] + w_specs,
                pl.BlockSpec((HALF, depth), whole), shape, (u, w_gate, w_up, w_down), scalars=(idx,), after=after,
                cost_estimate=cost(6 * HALF * depth * hidden, 6 * depth * hidden))


FINISH_ROWS = 64


def finish_rows(own_ref, got_ref, h_ref, gain_ref, o_ref, sums_ref):
    rows, width = o_ref.shape

    def squares(r):
        at = pl.ds(r, 16)
        total = None
        for cols in tiles(width):
            m = own_ref[at, cols] + got_ref[at, cols]
            total = m * m if total is None else total + m * m
        sums_ref[at, :] = total

    def apply(r):
        at = pl.ds(r, 16)
        inv = sums_ref[at, :]
        for cols in tiles(width):
            m = own_ref[at, cols] + got_ref[at, cols]
            o_ref[at, cols] = (h_ref[at, cols].astype(F32) + m * inv * gain_ref[:, cols]).astype(BF16)

    row_blocks(rows, 16, squares)
    to_inv_rms(sums_ref, rows, width)
    row_blocks(rows, 16, apply)


def finish_kernel(idx_ref, own_ref, got_ref, h_ref, gain_ref, o_ref, sums_ref):
    finish_rows(own_ref, got_ref, h_ref, gain_ref, o_ref, sums_ref)


def finish_place_kernel(idx_ref, own_ref, got_ref, h_ref, gain_ref, *rest):
    o_ref, all_ref, sums_ref = rest[-3:]
    finish_rows(own_ref, got_ref, h_ref, gain_ref, o_ref, sums_ref)
    all_ref[...] = o_ref[...]


def finish(idx, own, got, h, gain, after, place=None):
    width = own.shape[1]
    rows = FINISH_ROWS
    spec = pl.BlockSpec((rows, width), lambda i, idx: (i, 0))
    in_specs = [spec, spec, pl.BlockSpec((rows, width), lambda i, idx: (idx[1] * (HALF // rows) + i, 0)),
                pl.BlockSpec((1, width), lambda i, idx: (0, 0))]
    shape = jax.ShapeDtypeStruct((HALF, width), BF16)
    sums = [pltpu.VMEM((rows, LANES), F32)]
    estimate = cost(HALF * width * 1000, 12 * HALF * width)
    if place is None:
        return call(finish_kernel, (HALF // rows,), in_specs, spec, shape, (own, got, h, gain), scalars=(idx,), scratch=sums,
                    after=after, cost_estimate=estimate)
    out, total, chunk = place
    args, aliases = [own, got, h, gain], {}
    if out is not None:
        args.append(out)
        in_specs.append(pl.BlockSpec(memory_space=pl.ANY))
        aliases = {5: 1}
    at = pl.BlockSpec((rows, width), lambda i, idx: (chunk * (CHUNK // rows) + idx[1] * (HALF // rows) + i, 0))
    return call(finish_place_kernel, (HALF // rows,), in_specs, [spec, at],
                [shape, jax.ShapeDtypeStruct((total, width), BF16)], args, scalars=(idx,), scratch=sums, after=after, aliases=aliases,
                cost_estimate=estimate)


def place_kernel(idx_ref, half_ref, all_ref, out_ref):
    out_ref[...] = half_ref[...]


def place_peer(idx, half, out, chunk, after):
    width = half.shape[1]
    rows = FINISH_ROWS
    at = pl.BlockSpec((rows, width), lambda i, idx: (chunk * (CHUNK // rows) + (1 - idx[1]) * (HALF // rows) + i, 0))
    return call(place_kernel, (HALF // rows,),
                [pl.BlockSpec((rows, width), lambda i, idx: (i, 0)), pl.BlockSpec(memory_space=pl.ANY)], at,
                jax.ShapeDtypeStruct(out.shape, BF16), (half, out), scalars=(idx,), after=after, aliases={2: 0},
                cost_estimate=cost(HALF * width * 300, 4 * HALF * width))


def angles(positions, base):
    half = HEAD // 2
    inv_freq = base ** (-jnp.arange(half, dtype=F32) / half)
    angle = positions.astype(F32)[:, None] * inv_freq
    return jnp.cos(angle), jnp.sin(angle)


def solution(mesh):
    sp = mesh.shape['sp']
    swap = [(0, 1), (1, 0)]

    def shift(value, k):
        return lax.ppermute(value, 'sp', [(i, (i + k) % sp) for i in range(sp)])

    def other(value):
        return lax.ppermute(value, 'tp', swap)

    def device_fn(x, pos, gains, w_q, w_k, w_v, w_o, w_gate, w_up, w_down):
        s, t = lax.axis_index('sp'), lax.axis_index('tp')
        idx = jnp.stack([s, t]).astype(jnp.int32)
        chunks = x.shape[0] // CHUNK
        depth = x.shape[1]
        gain = lambda layer, i: gains[layer, i][None, :]
        w_o4 = w_o.reshape(2, sp, -1, depth)
        rows_o = w_o4.shape[2]
        last = []

        def run(fn, *args, **kw):
            used = [id(v) for v in jax.tree.leaves((args, kw))]
            out = fn(*args, after=tuple(v for v in last if id(v) not in used), **kw)
            last[:] = [out[0] if isinstance(out, (list, tuple)) else out]
            return out

        def gather_w_o(layer):
            mine = lax.dynamic_slice(w_o4, (layer, s, 0, 0), (1, 1, rows_o, depth)).reshape(rows_o, depth)
            got = other(mine)
            return [got] + [shift(got, -k) for k in range(1, sp)]

        def mlp_phase(layer, steps, tail, place):
            mids, sums, got, mine, theirs = [], [], [], [], []
            out = None

            def close(c):
                nonlocal out
                own = run(finish, idx, sums[c], got[c], mids[c][0], gain(layer, 3),
                          place=(out, x.shape[0], c) if place else None)
                if place:
                    own, out = own
                mine.append(own)
                theirs.append(other(own))

            def put(c):
                nonlocal out
                out = run(place_peer, idx, theirs[c], out, c)

            def late(c):
                tail(c, mine, theirs) if tail else put(c)

            end = chunks - 1
            for c in range(chunks):
                mids.append(run(o_project, *steps(c)))
                if c == end and c > 0:
                    close(c - 1)
                mlp_of = lambda **kw: run(mlp, idx, mids[c][1], w_gate, w_up, w_down, layer, **kw)
                if c in (0, end):
                    got.append(other(mlp_of(half='peer')))
                    sums.append(mlp_of(half='own'))
                else:
                    own, peer = mlp_of()
                    sums.append(own)
                    got.append(other(peer))
                    close(c - 1)
                if 2 <= c:
                    late(c - 2)
            close(end)
            late(end - 1)
            late(end)
            return mine, theirs, out

        end = chunks - 1
        w_peer0 = gather_w_o(0)
        wide0 = run(regroup, w_q, w_k, w_v, 0)
        cos0, sin0 = angles(pos, LOCAL_BASE)
        project = lambda c: run(qkv0, x, gain(0, 0), cos0, sin0, wide0, sp, c, 1)
        q_tail, kv_tail = project(end)
        prev = shift(kv_tail, 1)

        tails = [kv_tail[:, g * 2 * HEAD:(g + 1) * 2 * HEAD] for g in range(sp)]
        local_kv = jnp.where(s == sp - 1, tails[sp - 1], jnp.zeros_like(tails[0]))
        for g in range(sp - 1):
            local_kv = local_kv + lax.ppermute(tails[g], 'sp', [(sp - 1, g)])

        attn, attn_peer = [], []
        for c in range(chunks):
            q, kv = project(c) if c < end else (q_tail, kv_tail)
            attn.append(run(local_attention, idx, q, prev, kv, sp, c))
            attn_peer.append(other(attn[c]))
            prev = kv
        wide1 = run(regroup, w_q, w_k, w_v, 1)
        cos1, sin1 = angles(lax.optimization_barrier((pos, attn[end]))[0], GLOBAL_BASE)
        w_peer1 = gather_w_o(1)
        received = []

        def to_heads(c, mine, theirs):
            blocks = run(qkv1, idx, mine[c], theirs[c], gain(1, 0), cos1, sin1, wide1, sp, c)
            received.append([blocks[0]] + [shift(blocks[k], k) for k in range(1, sp)])

        mine, theirs, _ = mlp_phase(
            0, lambda c: (idx, attn[c], attn_peer[c], w_o4, 0, w_peer0, x, c, gain(0, 1), gain(0, 2)), to_heads, False)

        owns, peers = [], []
        for c in range(chunks):
            outs = run(global_attention, idx, received, c, c == 0)
            if c == 0:
                k_global, v_global = outs[sp:]
            owns.append([outs[0]] + [shift(outs[k], -k) for k in range(1, sp)])
            peers.append([other(a) for a in owns[c]])
        _, _, out = mlp_phase(
            1, lambda c: (idx, owns[c], peers[c], w_o4, 1, w_peer1, (mine[c], theirs[c]), c, gain(1, 1), gain(1, 2)), None, True)
        cache = lambda value: value[:, None, :]
        return out, cache(local_kv[:, :HEAD]), cache(local_kv[:, HEAD:]), cache(k_global), cache(v_global)

    token_spec = P(('rep', 'sp'), None)
    cache_spec = P('rep', ('tp', 'sp'), None)
    in_specs = (token_spec, P(('rep', 'sp')), P(), P(None, None, 'tp', None), P(None, None, 'tp', None),
                P(None, None, 'tp', None), P(None, 'tp', None, None), P(None, None, 'tp'), P(None, None, 'tp'),
                P(None, 'tp', None))
    out_specs = (token_spec, cache_spec, cache_spec, cache_spec, cache_spec)

    step = jax.shard_map(device_fn, mesh=mesh, in_specs=in_specs, out_specs=out_specs, check_vma=False)

    def program(*args):
        jax.eval_shape(step, *args)
        return step(*args)

    return program
```
